32 devices in a mesh: group: 2 (over x), ctx: 8 (over z, y), tp: 2 (over core).
Axes of the slice: x: 2, y: 2, z: 4, core: 2. Of those that a mesh axis runs over, the one named last changes fastest.
Arguments:
- stretch_query: bfloat16 [2, 1024, 8192], P('group', 'ctx', 'tp'), may hold values from -8 to 8
- prefix_keyvals: bfloat16 [2, 2, 8192, 1024], P('group', None, 'ctx', 'tp'), may hold values from -6 to 6
- stretch_key_values: bfloat16 [2, 2, 1024, 1024], P('group', None, 'ctx', 'tp'), may hold values from -6 to 6
- stretch_start: int32 [2], P('group'), may hold values from 2048 to 8192
- decode_query: bfloat16 [256, 4, 8192], P(('group', 'ctx'), None, 'tp'), may hold values from -8 to 8
- draft_key_values: bfloat16 [2, 256, 4, 1024], P(None, ('group', 'ctx'), None, 'tp'), may hold values from -6 to 6
- decode_cache: bfloat16 [2, 256, 1024, 1024], P(None, ('group', 'ctx'), None, 'tp'), may hold values from -6 to 6
- cache_lengths: int32 [256], P(('group', 'ctx')), may hold values from 128 to 1024, as said below
- page_rows: int32 [16], replicated, may hold values from 0 to 255, as said below
Outputs:
- prefill_out: bfloat16 [2, 1024, 8192], P('group', 'ctx', 'tp')
- decode_out: bfloat16 [256, 4, 8192], P(('group', 'ctx'), None, 'tp')
The draws below stay inside these ranges and needn't reach their ends.
Inputs may be any that keep to these rules, and one draw needn't show every extreme that they name: `cache_lengths`: one row has length 1024. `page_rows`: page n = g * 8 + c names one of the rows m * 16 to m * 16 + 15, where m = (n + 1) mod 16 if n mod 4 = 1, m = g * 8 + (c + 8 / 2) mod 8 if n mod 4 = 3, and m = (n + 8) mod 16 for even n; no row is named twice.
All inputs are finite; a program needn't handle non-finite values.
Results may differ from the reference program's by a relative error of at most 0.0049.
Values may be sent and summed in bfloat16 or wider, within the bound.
A program may use at most 128 MiB of HBM per device.

```python
import math
import jax
import jax.numpy as jnp
from jax import lax

QUERY_HEADS = 64
KEY_VALUE_HEADS = 8
HEAD_SIZE = 128
STRETCH_DEV = 128
ROWS_DEV = 16
ROW_CACHE_LIMIT = 1024
DRAFT_TOKENS = 4
QUERY_GROUP = 8
PREFILL_COUNT = 2
STRETCH_LENGTH = 1024
PREFIX_LENGTH = 8192
DECODE_ROWS = 256
PAGES = 16
N_CTX = 8


def draw_stretch_query(key, part):
    local = jax.random.fold_in(key, 11)
    values = jnp.clip(2.5 * jax.random.normal(local, (PREFILL_COUNT, STRETCH_LENGTH, QUERY_HEADS * HEAD_SIZE), jnp.float32), -8.0, 8.0)
    return values.astype(jnp.bfloat16)


def draw_prefix_keyvals(key, part):
    local = jax.random.fold_in(key, 21)
    array_shape = (PREFILL_COUNT, 2, PREFIX_LENGTH, KEY_VALUE_HEADS * HEAD_SIZE)
    values = jnp.clip(jax.random.normal(local, array_shape, jnp.float32), -6.0, 6.0)
    return values.astype(jnp.bfloat16)


def draw_decode_query(key, part):
    local = jax.random.fold_in(key, 31)
    array_shape = (DECODE_ROWS, DRAFT_TOKENS, QUERY_HEADS * HEAD_SIZE)
    values = jnp.clip(2.5 * jax.random.normal(local, array_shape, jnp.float32), -8.0, 8.0)
    return values.astype(jnp.bfloat16)


def draw_decode_cache(key, part):
    local = jax.random.fold_in(key, 41)
    array_shape = (2, DECODE_ROWS, ROW_CACHE_LIMIT, KEY_VALUE_HEADS * HEAD_SIZE)
    values = jnp.clip(jax.random.normal(local, array_shape, jnp.float32), -6.0, 6.0)
    return values.astype(jnp.bfloat16)


def draw_cache_lengths(key, part):
    blocks = DECODE_ROWS // ROWS_DEV
    levels = (ROW_CACHE_LIMIT // STRETCH_DEV).bit_length() - 1
    power = jax.random.randint(jax.random.fold_in(key, 51), (blocks, 1), 0, levels + 1)
    ceiling = STRETCH_DEV * 2 ** power
    spread = jax.random.randint(jax.random.fold_in(key, 52), (blocks, ROWS_DEV), 0, ceiling - STRETCH_DEV + 1)
    lengths = (STRETCH_DEV + spread).reshape(DECODE_ROWS)
    longest = jax.random.randint(jax.random.fold_in(key, 53), (), 0, DECODE_ROWS)
    lengths = jnp.where(jnp.arange(DECODE_ROWS) == longest, ROW_CACHE_LIMIT, lengths)
    return lengths.astype(jnp.int32)


def draw_page_rows(key, part):
    page_ids = jnp.arange(PAGES, dtype=jnp.int32)
    kind = page_ids % 4
    odd_page = page_ids % 2 == 1
    position = page_ids % N_CTX
    half_away = page_ids - position + (position + N_CTX // 2) % N_CTX
    target_block = jnp.where(kind == 1, page_ids + 1, jnp.where(kind == 3, half_away, page_ids + PAGES // 2)) % PAGES
    first_row = jax.random.randint(jax.random.fold_in(key, 61), (PAGES,), 0, ROWS_DEV)
    second_row = (first_row + 1 + jax.random.randint(jax.random.fold_in(key, 62), (PAGES,), 0, ROWS_DEV - 1)) % ROWS_DEV
    within = jnp.where(odd_page, first_row[target_block], second_row[target_block])
    return (target_block * ROWS_DEV + within).astype(jnp.int32)


def level_of(stream_key, shape, pieces, low, largest):
    loudness = 1.0
    for axis_at, shards_of in pieces:
        steps = jax.random.uniform(jax.random.fold_in(jax.random.fold_in(stream_key, 6), axis_at), (shards_of,), jnp.float32, low / len(pieces), largest / len(pieces))
        loudness = loudness * jnp.repeat(jnp.exp(steps), shape[axis_at] // shards_of).reshape((-1,) + (1,) * (len(shape) - 1 - axis_at))
    return loudness


def gaussian(own_key, dims, scale, most, split=(), kind=jnp.bfloat16):
    gain = level_of(own_key, dims, split, -0.22, 0.18) if split else 1.0
    drawn = jax.random.normal(own_key, dims, jnp.float32) * scale * gain
    return jnp.minimum(jnp.maximum(drawn, -most), most).astype(kind)


def setup_inputs(seed: int = 0) -> dict:
    streams_of = jax.random.split(jax.random.key(seed), 10)
    stretch_query = draw_stretch_query(jax.random.fold_in(streams_of[9], 71), 0)
    prefix_keyvals = draw_prefix_keyvals(jax.random.fold_in(streams_of[9], 71), 0)
    stretch_key_values = gaussian(streams_of[2], (PREFILL_COUNT, 2, STRETCH_LENGTH, KEY_VALUE_HEADS * HEAD_SIZE), 1.0, 6.0, ((0, 2), (2, 8), (3, 2)))
    stretch_start = jax.random.randint(streams_of[3], (PREFILL_COUNT,), PREFIX_LENGTH // 4, PREFIX_LENGTH + 1).astype(jnp.int32)
    decode_query = draw_decode_query(jax.random.fold_in(streams_of[9], 71), 0)
    draft_key_values = gaussian(streams_of[5], (2, DECODE_ROWS, DRAFT_TOKENS, KEY_VALUE_HEADS * HEAD_SIZE), 1.0, 6.0, ((1, 16), (3, 2)))
    decode_cache = draw_decode_cache(jax.random.fold_in(streams_of[9], 71), 0)
    cache_lengths = draw_cache_lengths(jax.random.fold_in(streams_of[9], 71), 0)
    page_rows = draw_page_rows(jax.random.fold_in(streams_of[9], 71), 0)
    return dict(stretch_query=stretch_query, prefix_keyvals=prefix_keyvals, stretch_key_values=stretch_key_values, stretch_start=stretch_start, decode_query=decode_query, draft_key_values=draft_key_values, decode_cache=decode_cache, cache_lengths=cache_lengths, page_rows=page_rows)


def attend_rows(queries, rows_of_keys, rows_of_values, allowed):
    scores = jnp.dot(queries, rows_of_keys.T, preferred_element_type=jnp.float32) * (1.0 / math.sqrt(HEAD_SIZE))
    masked = jnp.where(allowed, scores, -jnp.inf)
    highest = lax.optimization_barrier(jnp.max(masked, axis=-1, keepdims=True))
    weights = jnp.exp(masked - highest)
    totals = lax.optimization_barrier(jnp.sum(weights, axis=-1, keepdims=True))
    summed = jnp.dot(weights.astype(jnp.bfloat16), rows_of_values, preferred_element_type=jnp.float32)
    return (summed / totals).astype(jnp.bfloat16)

def prefill_request(query, prefix_length, stretch_length, limit):
    total_length = PREFIX_LENGTH + STRETCH_LENGTH
    heads_q = query.reshape(STRETCH_LENGTH, QUERY_HEADS, HEAD_SIZE).transpose(1, 0, 2)
    joined_keys = jnp.concatenate([prefix_length[0], stretch_length[0]], axis=0).reshape(total_length, KEY_VALUE_HEADS, HEAD_SIZE).transpose(1, 0, 2)
    joined_values = jnp.concatenate([prefix_length[1], stretch_length[1]], axis=0).reshape(total_length, KEY_VALUE_HEADS, HEAD_SIZE).transpose(1, 0, 2)
    key_pos = jnp.arange(total_length, dtype=jnp.int32)
    query_pos = jnp.arange(STRETCH_LENGTH, dtype=jnp.int32)
    allowed = jnp.where(key_pos[None, :] < PREFIX_LENGTH, key_pos[None, :] < limit, (key_pos - PREFIX_LENGTH)[None, :] <= query_pos[:, None])

    def one_head(head_index):
        kv_index = head_index // QUERY_GROUP
        return attend_rows(heads_q[head_index], joined_keys[kv_index], joined_values[kv_index], allowed)
    result = lax.map(one_head, jnp.arange(QUERY_HEADS, dtype=jnp.int32))
    return result.transpose(1, 0, 2).reshape(STRETCH_LENGTH, QUERY_HEADS * HEAD_SIZE)

def reference(stretch_query, prefix_keyvals, stretch_key_values, stretch_start, decode_query, draft_key_values, decode_cache, cache_lengths, page_rows):
    results = []
    for request in range(PREFILL_COUNT):
        results.append(prefill_request(stretch_query[request], prefix_keyvals[request], stretch_key_values[request], stretch_start[request]))
    prefill_out = jnp.stack(results)
    column_count = KEY_VALUE_HEADS * HEAD_SIZE
    pages = stretch_key_values.reshape(PREFILL_COUNT, 2, N_CTX, STRETCH_DEV, column_count).transpose(0, 2, 1, 3, 4).reshape(PAGES, 2, STRETCH_DEV, column_count)
    token_span = ROW_CACHE_LIMIT + DRAFT_TOKENS
    key_pos = jnp.arange(token_span, dtype=jnp.int32)
    step_pos = jnp.arange(DRAFT_TOKENS, dtype=jnp.int32)

    def one_row(row_index):
        matches = page_rows == row_index
        has_page = jnp.any(matches)
        page_block = jnp.einsum('p,pcsd->csd', matches.astype(jnp.float32), pages.astype(jnp.float32)).astype(jnp.bfloat16)
        row_cache = decode_cache[:, row_index]
        head_part = jnp.where(has_page, page_block, row_cache[:, :STRETCH_DEV])
        fresh = draft_key_values[:, row_index]
        rows_of_keys = jnp.concatenate([head_part[0], row_cache[0, STRETCH_DEV:], fresh[0]], axis=0)
        rows_of_values = jnp.concatenate([head_part[1], row_cache[1, STRETCH_DEV:], fresh[1]], axis=0)
        heads_of_keys = jnp.repeat(rows_of_keys.reshape(token_span, KEY_VALUE_HEADS, HEAD_SIZE).transpose(1, 0, 2), QUERY_GROUP, axis=0)
        heads_of_values = jnp.repeat(rows_of_values.reshape(token_span, KEY_VALUE_HEADS, HEAD_SIZE).transpose(1, 0, 2), QUERY_GROUP, axis=0)
        allowed = jnp.where(key_pos[None, :] < ROW_CACHE_LIMIT, key_pos[None, :] < cache_lengths[row_index], (key_pos - ROW_CACHE_LIMIT)[None, :] <= step_pos[:, None])
        heads_q = decode_query[row_index].reshape(DRAFT_TOKENS, QUERY_HEADS, HEAD_SIZE).transpose(1, 0, 2)
        result = jax.vmap(attend_rows, in_axes=(0, 0, 0, None))(heads_q, heads_of_keys, heads_of_values, allowed)
        return result.transpose(1, 0, 2).reshape(DRAFT_TOKENS, QUERY_HEADS * HEAD_SIZE)
    decode_out = lax.map(one_row, jnp.arange(DECODE_ROWS, dtype=jnp.int32))
    return (prefill_out, decode_out)
```

```python
import functools
import math

import jax
import jax.numpy as jnp
from jax import lax
from jax.experimental import pallas as pl
from jax.experimental.pallas import tpu as pltpu
from jax.sharding import PartitionSpec as P

QUERY_HEADS = 64
KEY_VALUE_HEADS = 8
HEAD_SIZE = 128
QUERY_GROUP = QUERY_HEADS // KEY_VALUE_HEADS
SCALE2 = math.log2(math.e) / math.sqrt(HEAD_SIZE)
LOW = -1e30
MESH = pl.DeviceIdType.MESH


def nt(a, b):
    return lax.dot_general(a, b, (((1,), (1,)), ((), ())), preferred_element_type=jnp.float32)


def tn(a, b):
    return lax.dot_general(a, b, (((0,), (0,)), ((), ())), preferred_element_type=jnp.float32)


def decode_kernel(
    heads, steps, page_size, info, q_ref, cache_ref, draft_ref, even_ref, odd_ref, out_ref, wide
):
    row = pl.program_id(0)
    length = info[row]
    rows_per_head = QUERY_GROUP * steps
    lanes = heads * rows_per_head

    @pl.when(row == 0)
    def _():
        wide[...] = jnp.zeros_like(wide)

    for h in range(heads):
        wide[h * rows_per_head : (h + 1) * rows_per_head, h * HEAD_SIZE : (h + 1) * HEAD_SIZE] = (
            q_ref[0, h]
        )
    queries = wide[...]
    row_count = pl.num_programs(0)
    is_even = info[row_count] == row
    is_odd = info[row_count + 1] == row

    def first(part):
        here = cache_ref[part, 0, :page_size, :]
        return jnp.where(is_even, even_ref[part], jnp.where(is_odd, odd_ref[part], here))

    positions = cache_ref.shape[2]
    rest = positions - page_size
    s0 = nt(first(0), queries)
    s1 = nt(cache_ref[0, 0, page_size:, :], queries)
    s2 = nt(draft_ref[0, 0], queries)
    pos0 = lax.broadcasted_iota(jnp.int32, (page_size, lanes), 0)
    pos1 = lax.broadcasted_iota(jnp.int32, (rest, lanes), 0) + page_size
    pos2 = lax.broadcasted_iota(jnp.int32, s2.shape, 0)
    step = lax.broadcasted_iota(jnp.int32, s2.shape, 1) % steps
    s0 = jnp.where(pos0 < length, s0, -jnp.inf)
    s1 = jnp.where(pos1 < length, s1, -jnp.inf)
    s2 = jnp.where(pos2 <= step, s2, -jnp.inf)
    top = jnp.maximum(
        jnp.maximum(jnp.max(s0, axis=0, keepdims=True), jnp.max(s1, axis=0, keepdims=True)),
        jnp.max(s2, axis=0, keepdims=True),
    )
    anchor = top * SCALE2
    w0 = jnp.exp2(s0 * SCALE2 - anchor)
    w1 = jnp.exp2(s1 * SCALE2 - anchor)
    w2 = jnp.exp2(s2 * SCALE2 - anchor)
    total = (
        jnp.sum(w0, axis=0, keepdims=True)
        + jnp.sum(w1, axis=0, keepdims=True)
        + jnp.sum(w2, axis=0, keepdims=True)
    )
    summed = tn(w0.astype(jnp.bfloat16), first(1))
    summed += tn(w1.astype(jnp.bfloat16), cache_ref[1, 0, page_size:, :])
    summed += tn(w2.astype(jnp.bfloat16), draft_ref[1, 0])
    inverse = jnp.broadcast_to(1.0 / total, (8, lanes)).T[:, :1]
    summed = summed * inverse
    for h in range(heads):
        out_ref[0, h] = summed[
            h * rows_per_head : (h + 1) * rows_per_head, h * HEAD_SIZE : (h + 1) * HEAD_SIZE
        ].astype(jnp.bfloat16)


def decode(info, queries, cache, draft, even, odd, steps):
    row_count, heads, per_head, _ = queries.shape
    page_size = even.shape[1]
    columns = heads * HEAD_SIZE
    positions = cache.shape[2]
    pad = draft.shape[2]
    return pl.pallas_call(
        functools.partial(decode_kernel, heads, steps, page_size),
        grid_spec=pltpu.PrefetchScalarGridSpec(
            num_scalar_prefetch=1,
            grid=(row_count,),
            in_specs=[
                pl.BlockSpec((1, heads, per_head, HEAD_SIZE), lambda r, i: (r, 0, 0, 0)),
                pl.BlockSpec((2, 1, positions, columns), lambda r, i: (0, r, 0, 0)),
                pl.BlockSpec((2, 1, pad, columns), lambda r, i: (0, r, 0, 0)),
                pl.BlockSpec((2, page_size, columns), lambda r, i: (0, 0, 0)),
                pl.BlockSpec((2, page_size, columns), lambda r, i: (0, 0, 0)),
            ],
            out_specs=pl.BlockSpec((1, heads, per_head, HEAD_SIZE), lambda r, i: (r, 0, 0, 0)),
            scratch_shapes=[pltpu.VMEM((heads * per_head, columns), jnp.bfloat16)],
        ),
        out_shape=jax.ShapeDtypeStruct(queries.shape, jnp.bfloat16),
        cost_estimate=pl.CostEstimate(
            flops=4 * row_count * positions * columns * heads * per_head,
            bytes_accessed=cache.size * 2,
            transcendentals=row_count * positions * heads * per_head,
        ),
        name="decode_rows",
    )(info, queries, cache, draft, even, odd)


MASKED = -30000.0


def layout(n_ctx):
    width = 2 ** ((n_ctx.bit_length() - 1) // 2)
    return width, n_ctx // (2 * width)


def prefill_kernel(
    n_ctx, start_ref, q_hbm, prefix_hbm, stretch_hbm, out_ref,
    qb, kv, bias, turned, top, acc, sbuf, o_send, o_got, s_send, s_got,
    own_sem, q_sems, kv_sems, st_sems, o_sems, s_sems,
):
    width, deep = layout(n_ctx)
    members = width * deep
    me = lax.axis_index("ctx")
    side = me // members
    place = me % members
    line, column = place // width, place % width
    partner = (me + members) % n_ctx
    tokens = q_hbm.shape[0]
    heads = kv.shape[1]
    keys = prefix_hbm.shape[2]
    page = stretch_hbm.shape[2]
    q_wide = QUERY_GROUP * HEAD_SIZE

    def at_place(down, right):
        return lax.rem(line + down, deep) * width + lax.rem(column + right, width)

    def from_place(down, right):
        return lax.rem(line + deep - down, deep) * width + lax.rem(column + width - right, width)

    def device(where):
        return {"ctx": side * members + where}

    near = [(0, r) for r in range(1, width)] + [(d, 0) for d in range(1, deep)]
    far = [(d, r) for d in range(1, deep) for r in range(1, width)]

    barrier = pltpu.get_barrier_semaphore()
    for d, r in near:
        pl.semaphore_signal(
            barrier, inc=1, device_id=device(at_place(d, r)), device_id_type=MESH
        )
    pl.semaphore_signal(barrier, inc=1, device_id={"ctx": partner}, device_id_type=MESH)
    pl.semaphore_wait(barrier, len(near) + 1)

    def cols(h, size):
        return pl.ds(pl.multiple_of(h * size, size), size)

    def remote(src, dst, sems, index, to):
        return pltpu.make_async_remote_copy(
            src_ref=src, dst_ref=dst, send_sem=sems.at[(0,) + index],
            recv_sem=sems.at[(1,) + index], device_id=to, device_id_type=MESH,
        )

    def q_copy(h):
        return remote(
            q_hbm.at[:, cols(h, q_wide)], qb.at[1, h], q_sems, (h,), {"ctx": partner}
        )

    def direct(h, d, r):
        kind = d * width + r
        to = device(at_place(d, r))
        return (
            remote(
                prefix_hbm.at[0, :, :, cols(h, HEAD_SIZE)],
                kv.at[place, h, :, pl.ds(0, keys)], kv_sems, (h, kind), to,
            ),
            remote(
                stretch_hbm.at[0, :, :, cols(h, HEAD_SIZE)],
                kv.at[place, h, :, pl.ds(keys, page)], st_sems, (h, kind), to,
            ),
        )

    def relay(h, d, r):
        slot = from_place(d, 0)
        return remote(
            kv.at[slot, h], kv.at[slot, h], kv_sems, (h, d * width + r), device(at_place(0, r))
        )

    def own(h):
        return (
            pltpu.make_async_copy(
                q_hbm.at[:, cols(h, q_wide)], qb.at[0, h], own_sem.at[h, 0]
            ),
            pltpu.make_async_copy(
                prefix_hbm.at[0, :, :, cols(h, HEAD_SIZE)],
                kv.at[place, h, :, pl.ds(0, keys)], own_sem.at[h, 1],
            ),
            pltpu.make_async_copy(
                stretch_hbm.at[0, :, :, cols(h, HEAD_SIZE)],
                kv.at[place, h, :, pl.ds(keys, page)], own_sem.at[h, 2],
            ),
        )

    def o_copies(h):
        to = {"ctx": partner}
        return (
            remote(o_send.at[h], o_got.at[h], o_sems, (h,), to),
            remote(s_send.at[h], s_got.at[h], s_sems, (h,), to),
        )

    @pl.loop(0, heads)
    def _(h):
        q_copy(h).start()
        for d, r in near[::-1]:
            for copy in direct(h, d, r):
                copy.start()
        for copy in own(h):
            copy.start()

    start = start_ref[0]
    chunks = [(at, min(256, keys - at)) for at in range(0, keys, 256)] + [(keys, page)]
    top[...] = jnp.full(top.shape, LOW, jnp.float32)
    acc[...] = jnp.zeros(acc.shape, jnp.float32)

    def absorb(h, slot):
        source = side * members + slot
        left = start - source * keys
        row = lax.broadcasted_iota(jnp.int32, (keys + page, HEAD_SIZE), 0)
        lane = lax.broadcasted_iota(jnp.int32, (keys + page, HEAD_SIZE), 1)
        valid = jnp.logical_or(row < left, row >= keys)
        bias[...] = jnp.where(
            jnp.logical_or(valid, lane > 0), 0.0, MASKED
        ).astype(jnp.bfloat16)
        values = kv[slot, h, 1] * jnp.where(valid, 1.0, 0.0).astype(jnp.bfloat16)
        turned[:HEAD_SIZE, :] = values.T
        extra = (turned.shape[0] - HEAD_SIZE, keys + page)
        place_of = lax.broadcasted_iota(jnp.int32, extra, 1)
        turned[HEAD_SIZE:, :] = jnp.where(
            jnp.logical_or(place_of < left, place_of >= keys), 1.0, 0.0
        ).astype(jnp.bfloat16)
        token = lax.broadcasted_iota(jnp.int32, (page, 2 * tokens), 1)
        q_pos = jnp.where(token < tokens, me * tokens + token, partner * tokens + token - tokens)
        k_pos = source * page + lax.broadcasted_iota(jnp.int32, (page, 2 * tokens), 0)
        causal = k_pos <= q_pos
        ones = jnp.ones((2 * tokens, HEAD_SIZE), jnp.bfloat16)

        def queries(g):
            part = slice(g * HEAD_SIZE, (g + 1) * HEAD_SIZE)
            both = jnp.concatenate([qb[0, h, :, part], qb[1, h, :, part]], axis=0)
            return jnp.concatenate([both, ones], axis=1)

        def score(g, q, at, size):
            block = jnp.concatenate(
                [kv[slot, h, 0, at : at + size, :], bias[at : at + size, :]], axis=1
            )
            scores = nt(block, q)
            if at == keys:
                scores = jnp.where(causal, scores, LOW)
            sbuf[g % 2, at : at + size, :] = scores
            return jnp.max(scores.reshape(size // 8, 8, 2 * tokens), axis=0)

        peak = None
        q = queries(0)
        for at, size in chunks:
            found = score(0, q, at, size)
            peak = found if peak is None else jnp.maximum(peak, found)
        for g in range(QUERY_GROUP):
            old = top[h, g : g + 1, :]
            new = jnp.maximum(old, jnp.max(peak, axis=0, keepdims=True))
            anchor = new * SCALE2
            factor = jnp.exp2(old * SCALE2 - anchor)
            top[h, g : g + 1, :] = new
            peak, product = None, None
            if g + 1 < QUERY_GROUP:
                q = queries(g + 1)
            for at, size in chunks:
                if g + 1 < QUERY_GROUP:
                    found = score(g + 1, q, at, size)
                    peak = found if peak is None else jnp.maximum(peak, found)
                weights = jnp.exp2(sbuf[g % 2, at : at + size, :] * SCALE2 - anchor)
                part = jnp.dot(
                    turned[:, at : at + size], weights.astype(jnp.bfloat16),
                    preferred_element_type=jnp.float32,
                )
                product = part if product is None else product + part
            acc[h, g] = acc[h, g] * factor + product

    @pl.loop(0, heads)
    def _(h):
        for copy in own(h):
            copy.wait()
        q_copy(h).wait_recv()
        absorb(h, place)
        for d, r in near[::-1]:
            for copy in direct(h, d, r):
                copy.wait_recv()
            if d > 0:
                for right in range(1, width):
                    relay(h, d, right).start()
            absorb(h, from_place(d, r))

    @pl.loop(0, heads)
    def _(h):
        for d, r in far:
            relay(h, d, r).wait_recv()
            absorb(h, from_place(d, r))
        for g in range(QUERY_GROUP):
            total = acc[h, g, HEAD_SIZE : HEAD_SIZE + 1, tokens:]
            inverse = jnp.where(total > 0, 1.0 / total, 0.0)
            o_send[h, g] = (acc[h, g, :HEAD_SIZE, tokens:] * inverse).astype(jnp.bfloat16)
            s_send[h, 0, g : g + 1, :] = top[h, g : g + 1, tokens:]
            s_send[h, 1, g : g + 1, :] = total
        for copy in o_copies(h):
            copy.start()

    @pl.loop(0, heads)
    def _(h):
        for copy in o_copies(h):
            copy.wait_recv()
        for g in range(QUERY_GROUP):
            ma, mb = top[h, g : g + 1, :tokens], s_got[h, 0, g : g + 1, :]
            high = jnp.maximum(ma, mb)
            fa = jnp.exp2((ma - high) * SCALE2)
            wb = s_got[h, 1, g : g + 1, :] * jnp.exp2((mb - high) * SCALE2)
            inverse = 1.0 / (acc[h, g, HEAD_SIZE : HEAD_SIZE + 1, :tokens] * fa + wb)
            done = acc[h, g, :HEAD_SIZE, :tokens] * (fa * inverse)
            done += o_got[h, g].astype(jnp.float32) * (wb * inverse)
            out_ref[0, :, pl.ds(pl.multiple_of(h * q_wide + g * HEAD_SIZE, HEAD_SIZE), HEAD_SIZE)] = (
                done.T.astype(jnp.bfloat16)
            )

    @pl.loop(0, heads)
    def _(h):
        q_copy(h).wait_send()
        for d, r in near:
            for copy in direct(h, d, r):
                copy.wait_send()
        for d, r in far:
            relay(h, d, r).wait_send()
        for copy in o_copies(h):
            copy.wait_send()


def prefill(n_ctx, start, queries, prefix, stretch):
    tokens, columns = queries.shape
    keys, page = prefix.shape[2], stretch.shape[2]
    heads = prefix.shape[3] // HEAD_SIZE
    members = n_ctx // 2
    rows = keys + page
    dma = pltpu.SemaphoreType.DMA
    hbm = pl.BlockSpec(memory_space=pl.ANY)
    return pl.pallas_call(
        functools.partial(prefill_kernel, n_ctx),
        in_specs=[pl.BlockSpec(memory_space=pltpu.SMEM), hbm, hbm, hbm],
        out_specs=pl.BlockSpec(memory_space=pltpu.VMEM),
        out_shape=jax.ShapeDtypeStruct((1, tokens, columns), jnp.bfloat16),
        scratch_shapes=[
            pltpu.VMEM((2, heads, tokens, QUERY_GROUP * HEAD_SIZE), jnp.bfloat16),
            pltpu.VMEM((members, heads, 2, rows, HEAD_SIZE), jnp.bfloat16),
            pltpu.VMEM((rows, HEAD_SIZE), jnp.bfloat16),
            pltpu.VMEM((HEAD_SIZE + 16, rows), jnp.bfloat16),
            pltpu.VMEM((heads, QUERY_GROUP, 2 * tokens), jnp.float32),
            pltpu.VMEM((heads, QUERY_GROUP, HEAD_SIZE + 16, 2 * tokens), jnp.float32),
            pltpu.VMEM((2, rows, 2 * tokens), jnp.float32),
            pltpu.VMEM((heads, QUERY_GROUP, HEAD_SIZE, tokens), jnp.bfloat16),
            pltpu.VMEM((heads, QUERY_GROUP, HEAD_SIZE, tokens), jnp.bfloat16),
            pltpu.VMEM((heads, 2, QUERY_GROUP, tokens), jnp.float32),
            pltpu.VMEM((heads, 2, QUERY_GROUP, tokens), jnp.float32),
            dma((heads, 3)),
            dma((2, heads)),
            dma((2, heads, members)),
            dma((2, heads, members)),
            dma((2, heads)),
            dma((2, heads)),
        ],
        compiler_params=pltpu.CompilerParams(
            collective_id=0, has_side_effects=True, vmem_limit_bytes=48 * 2**20
        ),
        cost_estimate=pl.CostEstimate(
            flops=16 * heads * QUERY_GROUP * tokens * rows * members * HEAD_SIZE,
            bytes_accessed=prefix.size * 2 * members,
            transcendentals=2 * heads * QUERY_GROUP * tokens * rows * members,
        ),
        name="prefill",
    )(start, queries, prefix, stretch)


def on_device(
    groups,
    n_ctx,
    stretch_query,
    prefix_keyvals,
    stretch_key_values,
    stretch_start,
    decode_query,
    draft_key_values,
    decode_cache,
    cache_lengths,
    page_rows,
):
    me = lax.axis_index("ctx")
    where = lax.axis_index("group") * n_ctx + me
    heads = stretch_key_values.shape[3] // HEAD_SIZE

    page_count = groups * n_ctx
    even_pairs = [(n, (n + page_count // 2) % page_count) for n in range(0, page_count, 2)]
    odd_pairs = []
    for n in range(1, page_count, 2):
        g, c = divmod(n, n_ctx)
        odd_pairs.append(
            (n, (n + 1) % page_count if n % 4 == 1 else g * n_ctx + (c + n_ctx // 2) % n_ctx)
        )
    page_own = stretch_key_values[0]
    even = lax.ppermute(page_own, ("group", "ctx"), even_pairs)
    odd = lax.ppermute(page_own, ("group", "ctx"), odd_pairs)
    prefill_out = prefill(
        n_ctx, stretch_start, stretch_query[0], prefix_keyvals, stretch_key_values
    )

    row_count, steps = decode_query.shape[:2]
    even_from = [-1] * page_count
    odd_from = [-1] * page_count
    for n, m in even_pairs:
        even_from[m] = n
    for n, m in odd_pairs:
        odd_from[m] = n

    def local_row(table):
        page = jnp.asarray(table, jnp.int32)[where]
        row = page_rows[jnp.maximum(page, 0)] - where * row_count
        return jnp.where(page >= 0, row, -1)

    decode_info = jnp.concatenate(
        [cache_lengths, jnp.stack([local_row(even_from), local_row(odd_from)])]
    ).astype(jnp.int32)
    decode_heads = (
        decode_query.reshape(row_count, steps, heads, QUERY_GROUP, HEAD_SIZE)
        .transpose(0, 2, 3, 1, 4)
        .reshape(row_count, heads, QUERY_GROUP * steps, HEAD_SIZE)
    )
    pad = -(-steps // 16) * 16
    draft = jnp.pad(draft_key_values, ((0, 0), (0, 0), (0, pad - steps), (0, 0)))
    decoded = decode(decode_info, decode_heads, decode_cache, draft, even, odd, steps)
    decode_out = (
        decoded.reshape(row_count, heads, QUERY_GROUP, steps, HEAD_SIZE)
        .transpose(0, 3, 1, 2, 4)
        .reshape(row_count, steps, heads * QUERY_GROUP * HEAD_SIZE)
    )

    return (prefill_out, decode_out)


def solution(mesh):
    return jax.shard_map(
        functools.partial(on_device, mesh.shape["group"], mesh.shape["ctx"]),
        mesh=mesh,
        in_specs=(
            P("group", "ctx", "tp"),
            P("group", None, "ctx", "tp"),
            P("group", None, "ctx", "tp"),
            P("group"),
            P(("group", "ctx"), None, "tp"),
            P(None, ("group", "ctx"), None, "tp"),
            P(None, ("group", "ctx"), None, "tp"),
            P(("group", "ctx")),
            P(),
        ),
        out_specs=(P("group", "ctx", "tp"), P(("group", "ctx"), None, "tp")),
        check_vma=False,
    )
```

```python
import functools
import math

import jax
import jax.numpy as jnp
from jax import lax
from jax.experimental import pallas as pl
from jax.experimental.pallas import tpu as pltpu
from jax.sharding import PartitionSpec as P

QUERY_HEADS = 64
KEY_VALUE_HEADS = 8
HEAD_SIZE = 128
QUERY_GROUP = QUERY_HEADS // KEY_VALUE_HEADS
SCALE2 = math.log2(math.e) / math.sqrt(HEAD_SIZE)
LOW = -1e30
MESH = pl.DeviceIdType.MESH

def nt(a, b):
    return lax.dot_general(a, b, (((1,), (1,)), ((), ())), preferred_element_type=jnp.float32)


def tn(a, b):
    return lax.dot_general(a, b, (((0,), (0,)), ((), ())), preferred_element_type=jnp.float32)


MASKED = -30000.0


def layout(n_ctx):
    width = 2 ** ((n_ctx.bit_length() - 1) // 2)
    return width, n_ctx // (2 * width)


def attend_kernel(
    n_ctx, groups, start_ref, lengths_ref, rows_ref, q_hbm, prefix_hbm, stretch_hbm,
    dq_hbm, draft_hbm, cache_hbm, out_ref, decoded_ref,
    dq, draft, cache, pages, wide, qb, kv, bias, turned, top, acc, sbuf, o_send, o_got, s_send, s_got,
    own_sem, q_sems, kv_sems, st_sems, o_sems, s_sems, cache_sem, row_sem, page_sems,
):
    width, deep = layout(n_ctx)
    members = width * deep
    me = lax.axis_index("ctx")
    side = me // members
    place = me % members
    line, column = place // width, place % width
    partner = (me + members) % n_ctx
    tokens = q_hbm.shape[0]
    heads = kv.shape[1]
    keys = prefix_hbm.shape[2]
    page = stretch_hbm.shape[2]
    q_wide = QUERY_GROUP * HEAD_SIZE

    def at_place(down, right):
        return lax.rem(line + down, deep) * width + lax.rem(column + right, width)

    def from_place(down, right):
        return lax.rem(line + deep - down, deep) * width + lax.rem(column + width - right, width)

    def device(where):
        return {"ctx": side * members + where}

    near = [(0, r) for r in range(1, width)] + [(d, 0) for d in range(1, deep)]
    far = [(d, r) for d in range(1, deep) for r in range(1, width)]

    barrier = pltpu.get_barrier_semaphore()
    for d, r in near:
        pl.semaphore_signal(
            barrier, inc=1, device_id=device(at_place(d, r)), device_id_type=MESH
        )
    pl.semaphore_signal(barrier, inc=1, device_id={"ctx": partner}, device_id_type=MESH)
    page_count = groups * n_ctx
    group = lax.axis_index("group")
    number = group * n_ctx + me
    half_away = group * n_ctx + (me + n_ctx // 2) % n_ctx
    across = (number + page_count // 2) % page_count
    before = (number + page_count - 1) % page_count
    kind = number % 4
    is_even = number % 2 == 0

    def at_number(which):
        return {"group": which // n_ctx, "ctx": which % n_ctx}

    @pl.when(kind != 1)
    def _():
        pl.semaphore_signal(
            barrier, inc=1, device_id=at_number(jnp.where(is_even, across, half_away)),
            device_id_type=MESH,
        )

    @pl.when(kind == 2)
    def _():
        pl.semaphore_signal(barrier, inc=1, device_id=at_number(before), device_id_type=MESH)

    pl.semaphore_wait(barrier, len(near) + 2)

    def cols(h, size):
        return pl.ds(pl.multiple_of(h * size, size), size)

    def remote(src, dst, sems, index, to):
        return pltpu.make_async_remote_copy(
            src_ref=src, dst_ref=dst, send_sem=sems.at[(0,) + index],
            recv_sem=sems.at[(1,) + index], device_id=to, device_id_type=MESH,
        )

    def q_copy(h):
        return remote(
            q_hbm.at[:, cols(h, q_wide)], qb.at[1, h], q_sems, (h,), {"ctx": partner}
        )

    def direct(h, d, r):
        kind = d * width + r
        to = device(at_place(d, r))
        return (
            remote(
                prefix_hbm.at[0, :, :, cols(h, HEAD_SIZE)],
                kv.at[place, h, :, pl.ds(0, keys)], kv_sems, (h, kind), to,
            ),
            remote(
                stretch_hbm.at[0, :, :, cols(h, HEAD_SIZE)],
                kv.at[place, h, :, pl.ds(keys, page)], st_sems, (h, kind), to,
            ),
        )

    cut = (keys + page) // 9 // 16 * 16

    def relay_right(h, d, r):
        part = kv.at[from_place(d, 0), h, :, pl.ds(cut, keys + page - cut)]
        return remote(part, part, kv_sems, (h, d * width + r), device(at_place(0, r)))

    def relay_down(h, d, r):
        part = kv.at[from_place(0, r), h, :, pl.ds(0, cut)]
        return remote(part, part, st_sems, (h, d * width + r), device(at_place(d, 0)))

    def own(h):
        return (
            pltpu.make_async_copy(
                q_hbm.at[:, cols(h, q_wide)], qb.at[0, h], own_sem.at[h, 0]
            ),
            pltpu.make_async_copy(
                prefix_hbm.at[0, :, :, cols(h, HEAD_SIZE)],
                kv.at[place, h, :, pl.ds(0, keys)], own_sem.at[h, 1],
            ),
            pltpu.make_async_copy(
                stretch_hbm.at[0, :, :, cols(h, HEAD_SIZE)],
                kv.at[place, h, :, pl.ds(keys, page)], own_sem.at[h, 2],
            ),
        )

    def o_copies(h):
        to = {"ctx": partner}
        return (
            remote(o_send.at[h], o_got.at[h], o_sems, (h,), to),
            remote(s_send.at[h], s_got.at[h], s_sems, (h,), to),
        )

    page_slot = number % 2
    page_to = jnp.where(
        is_even, across, jnp.where(kind == 1, (number + 1) % page_count, half_away)
    )
    page_copy = remote(
        stretch_hbm.at[0], pages.at[page_slot], page_sems, (page_slot,), at_number(page_to)
    )
    row_count, steps = dq_hbm.shape[:2]
    depth = cache.shape[0]

    def row_copy(row):
        slot = lax.rem(row, depth)
        return pltpu.make_async_copy(cache_hbm.at[:, row], cache.at[slot], cache_sem.at[slot])

    query_copy = pltpu.make_async_copy(dq_hbm, dq, row_sem.at[0])
    draft_copy = pltpu.make_async_copy(draft_hbm, draft, row_sem.at[1])
    def issue(h):
        q_copy(h).start()
        for d, r in near[::-1]:
            for copy in direct(h, d, r):
                copy.start()

    issue(0)
    page_copy.start()
    for h in range(1, min(2, heads)):
        issue(h)

    @pl.loop(0, heads)
    def _(h):
        for copy in own(h):
            copy.start()

    query_copy.start()
    draft_copy.start()
    for row in range(depth - 1):
        row_copy(row).start()

    start = start_ref[0]
    chunks = [(at, min(256, keys - at)) for at in range(0, keys, 256)] + [(keys, page)]
    top[...] = jnp.full(top.shape, LOW, jnp.float32)
    acc[...] = jnp.zeros(acc.shape, jnp.float32)

    def absorb(h, slot):
        source = side * members + slot
        left = start - source * keys
        row = lax.broadcasted_iota(jnp.int32, (keys + page, HEAD_SIZE), 0)
        lane = lax.broadcasted_iota(jnp.int32, (keys + page, HEAD_SIZE), 1)
        valid = jnp.logical_or(row < left, row >= keys)
        bias[...] = jnp.where(
            jnp.logical_or(valid, lane > 0), 0.0, MASKED
        ).astype(jnp.bfloat16)
        values = kv[slot, h, 1] * jnp.where(valid, 1.0, 0.0).astype(jnp.bfloat16)
        turned[:HEAD_SIZE, :] = values.T
        extra = (turned.shape[0] - HEAD_SIZE, keys + page)
        place_of = lax.broadcasted_iota(jnp.int32, extra, 1)
        turned[HEAD_SIZE:, :] = jnp.where(
            jnp.logical_or(place_of < left, place_of >= keys), 1.0, 0.0
        ).astype(jnp.bfloat16)
        token = lax.broadcasted_iota(jnp.int32, (page, 2 * tokens), 1)
        q_pos = jnp.where(token < tokens, me * tokens + token, partner * tokens + token - tokens)
        k_pos = source * page + lax.broadcasted_iota(jnp.int32, (page, 2 * tokens), 0)
        causal = k_pos <= q_pos
        ones = jnp.ones((2 * tokens, HEAD_SIZE), jnp.bfloat16)

        def queries(g):
            part = slice(g * HEAD_SIZE, (g + 1) * HEAD_SIZE)
            both = jnp.concatenate([qb[0, h, :, part], qb[1, h, :, part]], axis=0)
            return jnp.concatenate([both, ones], axis=1)

        def score(g, q, at, size):
            block = jnp.concatenate(
                [kv[slot, h, 0, at : at + size, :], bias[at : at + size, :]], axis=1
            )
            scores = nt(block, q)
            if at == keys:
                scores = jnp.where(causal, scores, LOW)
            sbuf[g % 2, at : at + size, :] = scores
            return jnp.max(scores.reshape(size // 8, 8, 2 * tokens), axis=0)

        peak = None
        q = queries(0)
        for at, size in chunks:
            found = score(0, q, at, size)
            peak = found if peak is None else jnp.maximum(peak, found)
        for g in range(QUERY_GROUP):
            old = top[h, g : g + 1, :]
            new = jnp.maximum(old, jnp.max(peak, axis=0, keepdims=True))
            anchor = new * SCALE2
            factor = jnp.exp2(old * SCALE2 - anchor)
            top[h, g : g + 1, :] = new
            peak, product = None, None
            if g + 1 < QUERY_GROUP:
                q = queries(g + 1)
            for at, size in chunks:
                if g + 1 < QUERY_GROUP:
                    found = score(g + 1, q, at, size)
                    peak = found if peak is None else jnp.maximum(peak, found)
                weights = jnp.exp2(sbuf[g % 2, at : at + size, :] * SCALE2 - anchor)
                part = jnp.dot(
                    turned[:, at : at + size], weights.astype(jnp.bfloat16),
                    preferred_element_type=jnp.float32,
                )
                product = part if product is None else product + part
            acc[h, g] = acc[h, g] * factor + product

    even_row = jnp.where(is_even, rows_ref[across] - number * row_count, -1)
    odd_row = jnp.where(
        kind >= 2,
        rows_ref[jnp.where(kind == 2, before, half_away)] - number * row_count,
        -1,
    )
    per_head = QUERY_GROUP * steps
    lanes = heads * per_head
    wide[...] = jnp.zeros_like(wide)

    def padded(x):
        rest = jnp.zeros((16 - steps, x.shape[1]), jnp.float32)
        return jnp.concatenate([x.astype(jnp.float32), rest], axis=0).astype(jnp.bfloat16)

    def decode_row(row):
        row_copy(row).wait()

        @pl.when(row + depth - 1 < row_count)
        def _():
            row_copy(row + depth - 1).start()

        slot = lax.rem(row, depth)
        length = lengths_ref[row]
        for h in range(heads):
            pieces = [
                dq[row, :, (h * QUERY_GROUP + g) * HEAD_SIZE : (h * QUERY_GROUP + g + 1) * HEAD_SIZE]
                for g in range(QUERY_GROUP)
            ]
            stacked = jnp.concatenate([p.astype(jnp.float32) for p in pieces], axis=0)
            wide[h * per_head : (h + 1) * per_head, h * HEAD_SIZE : (h + 1) * HEAD_SIZE] = (
                stacked.astype(jnp.bfloat16)
            )
        queries = wide[...]

        def first(part):
            here = cache[slot, part, :page, :]
            return jnp.where(
                even_row == row, pages[0, part], jnp.where(odd_row == row, pages[1, part], here)
            )

        s0 = nt(first(0), queries)
        s1 = nt(cache[slot, 0, page:, :], queries)
        s2 = nt(padded(draft[0, row]), queries)
        pos0 = lax.broadcasted_iota(jnp.int32, s0.shape, 0)
        pos1 = lax.broadcasted_iota(jnp.int32, s1.shape, 0) + page
        pos2 = lax.broadcasted_iota(jnp.int32, s2.shape, 0)
        step = lax.broadcasted_iota(jnp.int32, s2.shape, 1) % steps
        s0 = jnp.where(pos0 < length, s0, -jnp.inf)
        s1 = jnp.where(pos1 < length, s1, -jnp.inf)
        s2 = jnp.where(pos2 <= step, s2, -jnp.inf)
        best = jnp.maximum(
            jnp.maximum(jnp.max(s0, axis=0, keepdims=True), jnp.max(s1, axis=0, keepdims=True)),
            jnp.max(s2, axis=0, keepdims=True),
        )
        anchor = best * SCALE2
        w0 = jnp.exp2(s0 * SCALE2 - anchor)
        w1 = jnp.exp2(s1 * SCALE2 - anchor)
        w2 = jnp.exp2(s2 * SCALE2 - anchor)
        total = (
            jnp.sum(w0, axis=0, keepdims=True)
            + jnp.sum(w1, axis=0, keepdims=True)
            + jnp.sum(w2, axis=0, keepdims=True)
        )
        summed = tn(w0.astype(jnp.bfloat16), first(1))
        summed += tn(w1.astype(jnp.bfloat16), cache[slot, 1, page:, :])
        summed += tn(w2.astype(jnp.bfloat16), padded(draft[1, row]))
        inverse = jnp.broadcast_to(1.0 / total, (8, lanes)).T[:, :1]
        summed = summed * inverse
        for h in range(heads):
            for g in range(QUERY_GROUP):
                at = h * per_head + g * steps
                out = (h * QUERY_GROUP + g) * HEAD_SIZE
                decoded_ref[row, :, out : out + HEAD_SIZE] = summed[
                    at : at + steps, h * HEAD_SIZE : (h + 1) * HEAD_SIZE
                ].astype(jnp.bfloat16)

    def decode_rows(begin, count):
        @pl.loop(0, count)
        def _(i):
            decode_row(begin + i)

    late = row_count // 4
    each = (row_count - late) // heads
    late = row_count - each * heads

    def await_pages():
        query_copy.wait()
        draft_copy.wait()

        @pl.when(is_even)
        def _():
            remote(
                stretch_hbm.at[0], pages.at[0], page_sems, (0,), at_number(page_to)
            ).wait_recv()

        @pl.when(kind >= 2)
        def _():
            remote(
                stretch_hbm.at[0], pages.at[1], page_sems, (1,), at_number(page_to)
            ).wait_recv()

    def finish(h):
        for d, r in far:
            relay_right(h, d, r).wait_recv()
            relay_down(h, d, r).wait_recv()
            absorb(h, from_place(d, r))
        for g in range(QUERY_GROUP):
            total = acc[h, g, HEAD_SIZE : HEAD_SIZE + 1, tokens:]
            inverse = jnp.where(total > 0, 1.0 / total, 0.0)
            o_send[h, g] = (acc[h, g, :HEAD_SIZE, tokens:] * inverse).astype(jnp.bfloat16)
            s_send[h, 0, g : g + 1, :] = top[h, g : g + 1, tokens:]
            s_send[h, 1, g : g + 1, :] = total
        for copy in o_copies(h):
            copy.start()

    @pl.loop(0, heads + 1)
    def _(h):
        @pl.when(h < heads)
        def _():
            for copy in own(h):
                copy.wait()
            q_copy(h).wait_recv()
            absorb(h, place)
            for d, r in near[::-1]:
                for copy in direct(h, d, r):
                    copy.wait_recv()
                if d > 0:
                    for right in range(1, width):
                        relay_right(h, d, right).start()
                else:
                    for down in range(1, deep):
                        relay_down(h, down, r).start()

            @pl.when(h + 2 < heads)
            def _():
                issue(h + 2)

            for d, r in near[::-1]:
                absorb(h, from_place(d, r))

        @pl.when(h > 0)
        def _():
            finish(h - 1)

        @pl.when(h == 0)
        def _():
            await_pages()

        @pl.when(h < heads)
        def _():
            decode_rows(h * each, each)

    decode_rows(row_count - late, late)

    @pl.loop(0, heads)
    def _(h):
        for copy in o_copies(h):
            copy.wait_recv()
        for g in range(QUERY_GROUP):
            ma, mb = top[h, g : g + 1, :tokens], s_got[h, 0, g : g + 1, :]
            high = jnp.maximum(ma, mb)
            fa = jnp.exp2((ma - high) * SCALE2)
            wb = s_got[h, 1, g : g + 1, :] * jnp.exp2((mb - high) * SCALE2)
            inverse = 1.0 / (acc[h, g, HEAD_SIZE : HEAD_SIZE + 1, :tokens] * fa + wb)
            done = acc[h, g, :HEAD_SIZE, :tokens] * (fa * inverse)
            done += o_got[h, g].astype(jnp.float32) * (wb * inverse)
            out_ref[0, :, pl.ds(pl.multiple_of(h * q_wide + g * HEAD_SIZE, HEAD_SIZE), HEAD_SIZE)] = (
                done.T.astype(jnp.bfloat16)
            )

    page_copy.wait_send()

    @pl.loop(0, heads)
    def _(h):
        q_copy(h).wait_send()
        for d, r in near:
            for copy in direct(h, d, r):
                copy.wait_send()
        for d, r in far:
            relay_right(h, d, r).wait_send()
            relay_down(h, d, r).wait_send()
        for copy in o_copies(h):
            copy.wait_send()


def attend(n_ctx, groups, start, lengths, rows, queries, prefix, stretch, dq, draft, cache):
    tokens, columns = queries.shape
    keys, page = prefix.shape[2], stretch.shape[2]
    kv_columns = prefix.shape[3]
    heads = kv_columns // HEAD_SIZE
    members = n_ctx // 2
    total = keys + page
    row_count, steps = dq.shape[:2]
    positions = cache.shape[2]
    dma = pltpu.SemaphoreType.DMA
    hbm = pl.BlockSpec(memory_space=pl.ANY)
    smem = pl.BlockSpec(memory_space=pltpu.SMEM)
    vmem = pl.BlockSpec(memory_space=pltpu.VMEM)
    return pl.pallas_call(
        functools.partial(attend_kernel, n_ctx, groups),
        in_specs=[smem] * 3 + [hbm] * 6,
        out_specs=[vmem, vmem],
        out_shape=[
            jax.ShapeDtypeStruct((1, tokens, columns), jnp.bfloat16),
            jax.ShapeDtypeStruct(dq.shape, jnp.bfloat16),
        ],
        scratch_shapes=[
            pltpu.VMEM(dq.shape, jnp.bfloat16),
            pltpu.VMEM(draft.shape, jnp.bfloat16),
            pltpu.VMEM((3, 2, positions, kv_columns), jnp.bfloat16),
            pltpu.VMEM((2, 2, page, kv_columns), jnp.bfloat16),
            pltpu.VMEM((heads * QUERY_GROUP * steps, kv_columns), jnp.bfloat16),
            pltpu.VMEM((2, heads, tokens, QUERY_GROUP * HEAD_SIZE), jnp.bfloat16),
            pltpu.VMEM((members, heads, 2, total, HEAD_SIZE), jnp.bfloat16),
            pltpu.VMEM((total, HEAD_SIZE), jnp.bfloat16),
            pltpu.VMEM((HEAD_SIZE + 16, total), jnp.bfloat16),
            pltpu.VMEM((heads, QUERY_GROUP, 2 * tokens), jnp.float32),
            pltpu.VMEM((heads, QUERY_GROUP, HEAD_SIZE + 16, 2 * tokens), jnp.float32),
            pltpu.VMEM((2, total, 2 * tokens), jnp.float32),
            pltpu.VMEM((heads, QUERY_GROUP, HEAD_SIZE, tokens), jnp.bfloat16),
            pltpu.VMEM((heads, QUERY_GROUP, HEAD_SIZE, tokens), jnp.bfloat16),
            pltpu.VMEM((heads, 2, QUERY_GROUP, tokens), jnp.float32),
            pltpu.VMEM((heads, 2, QUERY_GROUP, tokens), jnp.float32),
            dma((heads, 3)),
            dma((2, heads)),
            dma((2, heads, members)),
            dma((2, heads, members)),
            dma((2, heads)),
            dma((2, heads)),
            dma((3,)),
            dma((2,)),
            dma((2, 2)),
        ],
        compiler_params=pltpu.CompilerParams(
            collective_id=0, has_side_effects=True, vmem_limit_bytes=56 * 2**20
        ),
        cost_estimate=pl.CostEstimate(
            flops=16 * heads * QUERY_GROUP * tokens * total * members * HEAD_SIZE,
            bytes_accessed=prefix.size * 2 * members + cache.size * 2,
            transcendentals=2 * heads * QUERY_GROUP * tokens * total * members,
        ),
        name="attend",
    )(start, lengths, rows, queries, prefix, stretch, dq, draft, cache)


def on_device(
    groups,
    n_ctx,
    stretch_query,
    prefix_keyvals,
    stretch_key_values,
    stretch_start,
    decode_query,
    draft_key_values,
    decode_cache,
    cache_lengths,
    page_rows,
):
    prefill_out, decode_out = attend(
        n_ctx, groups, stretch_start, cache_lengths, page_rows, stretch_query[0],
        prefix_keyvals, stretch_key_values, decode_query, draft_key_values, decode_cache,
    )
    return (prefill_out, decode_out)


def solution(mesh):
    return jax.shard_map(
        functools.partial(on_device, mesh.shape["group"], mesh.shape["ctx"]),
        mesh=mesh,
        in_specs=(
            P("group", "ctx", "tp"),
            P("group", None, "ctx", "tp"),
            P("group", None, "ctx", "tp"),
            P("group"),
            P(("group", "ctx"), None, "tp"),
            P(None, ("group", "ctx"), None, "tp"),
            P(None, ("group", "ctx"), None, "tp"),
            P(("group", "ctx")),
            P(),
        ),
        out_specs=(P("group", "ctx", "tp"), P(("group", "ctx"), None, "tp")),
        check_vma=False,
    )
```
